32 devices in a mesh: kx: 4 (over z), ky: 4 (over y, x), kz: 2 (over core).
Axes of the slice: x: 2, y: 2, z: 4, core: 2. Of those that a mesh axis runs over, the one named last changes fastest.
Arguments:
- u_start: float32 [4, 4, 8, 2, 128, 128], P('kx', 'ky', 'kz'), may hold values from -1 to 1, as said below
- intersections: float32 [4, 4, 8, 12, 2, 128, 128], P('kx', 'ky', 'kz'), may hold values from -1.2 to 1.2, as said below
Outputs:
- u_final: float32 [4, 4, 8, 2, 128, 128], P('kx', 'ky', 'kz')
- centres: float32 [3, 3, 128], replicated
- spreads: float32 [3, 128], replicated
The draws below stay inside these ranges and needn't reach their ends.
Inputs may be any that keep to these rules, and one draw needn't show every extreme that they name: `u_start`: each U(k) is unitary up to float32 rounding and close to the identity: every diagonal entry of U(k) has magnitude 0.7 or more. `intersections`: every diagonal entry of every M(k,b) has magnitude 0.45 or more and a phase within 1.9 of zero.
All inputs are finite; a program needn't handle non-finite values.
Results may differ from the reference program's by a relative error of at most 0.0003.
Values sent between devices are 32-bit elements; how exact they have to be, the bound alone decides.
A program may use at most 128 MiB of HBM per device.

```python
import jax
import jax.numpy as jnp
from jax import lax

NW = 128
NBV = 12
ITERS = 3
NKX = 4
NKY = 4
NKZ = 8


OFFSETS = ((1, 1, 0), (1, -1, 0), (-1, 1, 0), (-1, -1, 0), (1, 0, 1), (1, 0, -1), (-1, 0, 1), (-1, 0, -1), (0, 1, 1), (0, 1, -1), (0, -1, 1), (0, -1, -1))


PRECISE = lax.Precision.HIGHEST


def random_entries(seed_key, dims, spread):
    return jax.random.normal(seed_key, dims, jnp.float32) * spread


def matmul_drawn(left, right):
    return jnp.einsum('...ij,...jk->...ik', left, right, precision=PRECISE)


def draw_u_start(key, part):
    dims = (NKX, NKY, NKZ, NW, NW)
    raw_real = random_entries(jax.random.fold_in(key, 3), dims, 0.02)
    raw_imag = random_entries(jax.random.fold_in(key, 5), dims, 0.02)
    gen_real = raw_real - jnp.swapaxes(raw_real, -1, -2)
    gen_imag = raw_imag + jnp.swapaxes(raw_imag, -1, -2)
    identity = jnp.broadcast_to(jnp.eye(NW, dtype=jnp.float32), dims)
    term_real = identity
    term_imag = jnp.zeros(dims, jnp.float32)
    total_real = identity
    total_imag = jnp.zeros(dims, jnp.float32)
    for order in range(1, 13):
        next_real = (matmul_drawn(term_real, gen_real) - matmul_drawn(term_imag, gen_imag)) / order
        next_imag = (matmul_drawn(term_real, gen_imag) + matmul_drawn(term_imag, gen_real)) / order
        term_real = next_real
        term_imag = next_imag
        total_real = total_real + term_real
        total_imag = total_imag + term_imag
    return jnp.stack([total_real, total_imag], axis=3)


def draw_intersections(key, part):
    dims = (NKX, NKY, NKZ, NBV, NW, NW)
    centre_draw = jax.random.uniform(jax.random.fold_in(key, 11), (3, NW), jnp.float32, -1.0, 1.0)
    offset_table = jnp.array(OFFSETS, jnp.float32)
    coherent = jnp.dot(offset_table, centre_draw, precision=PRECISE)
    slope = 0.5 + (jnp.arange(NKX, dtype=jnp.float32) + 0.5) / NKX
    noise = jax.random.uniform(jax.random.fold_in(key, 13), (NKX, NKY, NKZ, NBV, NW), jnp.float32, -0.4, 0.4)
    phases = -0.5 * slope[:, None, None, None, None] * coherent[None, None, None] + noise
    magnitude = jax.random.uniform(jax.random.fold_in(key, 15), (NKX, NKY, NKZ, NBV, NW), jnp.float32, 0.6, 1.0)
    off_real = random_entries(jax.random.fold_in(key, 17), dims, 0.03)
    off_imag = random_entries(jax.random.fold_in(key, 19), dims, 0.03)
    identity = jnp.eye(NW, dtype=jnp.float32)
    outside = 1.0 - identity
    over_real = off_real * outside + identity * (magnitude * jnp.cos(phases))[..., None, :]
    over_imag = off_imag * outside + identity * (magnitude * jnp.sin(phases))[..., None, :]
    return jnp.stack([over_real, over_imag], axis=4)


def setup_inputs(seed: int = 0) -> dict:
    key_list = jax.random.split(jax.random.key(seed), 3)
    u_start = draw_u_start(jax.random.fold_in(key_list[2], 71), 0)
    intersections = draw_intersections(jax.random.fold_in(key_list[2], 71), 0)
    return dict(u_start=u_start, intersections=intersections)


OFFSETS = ((1, 1, 0), (1, -1, 0), (-1, 1, 0), (-1, -1, 0), (1, 0, 1), (1, 0, -1), (-1, 0, 1), (-1, 0, -1), (0, 1, 1), (0, 1, -1), (0, -1, 1), (0, -1, -1))
WEIGHT = 0.125
STEP_SIZE = 0.35
PRECISE = lax.Precision.HIGHEST


def matmul(left, right):
    return jnp.einsum('...ij,...jk->...ik', left, right, precision=PRECISE)


def adjoint_product(left, right):
    return jnp.einsum('...ji,...jk->...ik', left, right, precision=PRECISE)


def complex_product(left_real, left_imag, right_real, right_imag):
    return (matmul(left_real, right_real) - matmul(left_imag, right_imag),
            matmul(left_real, right_imag) + matmul(left_imag, right_real))


def reference(u_start, intersections):
    total_points = NKX * NKY * NKZ
    offset_table = jnp.array(OFFSETS, jnp.float32)
    identity = jnp.eye(NW, dtype=jnp.float32)
    unitary = u_start
    centre_list = []
    spread_list = []
    for iteration in range(ITERS):
        local_real = unitary[:, :, :, 0]
        local_imag = unitary[:, :, :, 1]
        records = []
        first_sums = jnp.zeros((3, NW), jnp.float32)
        second_sums = jnp.zeros((NW,), jnp.float32)
        for vector_index in range(NBV):
            offset = OFFSETS[vector_index]
            nearby = jnp.roll(unitary, (-offset[0], -offset[1], -offset[2]), axis=(0, 1, 2))
            intersection_real = intersections[:, :, :, vector_index, 0]
            intersection_imag = intersections[:, :, :, vector_index, 1]
            left_real = adjoint_product(local_real, intersection_real) + adjoint_product(local_imag, intersection_imag)
            left_imag = adjoint_product(local_real, intersection_imag) - adjoint_product(local_imag, intersection_real)
            turned_real, turned_imag = complex_product(left_real, left_imag, nearby[:, :, :, 0], nearby[:, :, :, 1])
            diagonal_real = jnp.diagonal(turned_real, axis1=-2, axis2=-1)
            diagonal_imag = jnp.diagonal(turned_imag, axis1=-2, axis2=-1)
            phases = jnp.arctan2(diagonal_imag, diagonal_real)
            magnitude = diagonal_real * diagonal_real + diagonal_imag * diagonal_imag
            first_sums = first_sums + WEIGHT * offset_table[vector_index][:, None] * jnp.sum(phases, axis=(0, 1, 2))[None, :]
            second_sums = second_sums + WEIGHT * jnp.sum(1.0 - magnitude + phases * phases, axis=(0, 1, 2))
            records.append((turned_real, turned_imag, diagonal_real, diagonal_imag, phases, magnitude))
        centres = -first_sums / total_points
        spreads = second_sums / total_points - jnp.sum(centres * centres, axis=0)
        centre_list.append(centres)
        spread_list.append(spreads)
        summed_real = jnp.zeros((NKX, NKY, NKZ, NW, NW), jnp.float32)
        summed_imag = jnp.zeros((NKX, NKY, NKZ, NW, NW), jnp.float32)
        for vector_index in range(NBV):
            turned_real, turned_imag, diagonal_real, diagonal_imag, phases, magnitude = records[vector_index]
            shifted = phases + jnp.sum(offset_table[vector_index][:, None] * centres, axis=0)
            scaled = (shifted / magnitude)[..., None, :]
            product_real = turned_real * diagonal_real[..., None, :] + turned_imag * diagonal_imag[..., None, :]
            product_imag = turned_imag * diagonal_real[..., None, :] - turned_real * diagonal_imag[..., None, :]
            summed_real = summed_real + (product_real - product_imag * scaled)
            summed_imag = summed_imag + (product_imag + product_real * scaled)
        gradient_real = 2.0 * WEIGHT * (summed_real - jnp.swapaxes(summed_real, -1, -2))
        gradient_imag = 2.0 * WEIGHT * (summed_imag + jnp.swapaxes(summed_imag, -1, -2))
        change_real = STEP_SIZE * gradient_real
        change_imag = STEP_SIZE * gradient_imag
        inner_real = 0.5 * identity + change_real / 6.0
        inner_imag = change_imag / 6.0
        middle_real, middle_imag = complex_product(change_real, change_imag, inner_real, inner_imag)
        middle_real = identity + middle_real
        exponent_real, exponent_imag = complex_product(change_real, change_imag, middle_real, middle_imag)
        exponent_real = identity + exponent_real
        update_real, update_imag = complex_product(local_real, local_imag, exponent_real, exponent_imag)
        unitary = jnp.stack([update_real, update_imag], axis=3)
    return unitary, jnp.stack(centre_list), jnp.stack(spread_list)
```

```python
import functools

import jax
import jax.numpy as jnp
from jax import lax
from jax.experimental import pallas as pl
from jax.experimental.pallas import tpu as pltpu
from jax.sharding import PartitionSpec as P

ITERS = 3


OFFSETS = (
    (1, 1, 0),
    (1, -1, 0),
    (-1, 1, 0),
    (-1, -1, 0),
    (1, 0, 1),
    (1, 0, -1),
    (-1, 0, 1),
    (-1, 0, -1),
    (0, 1, 1),
    (0, 1, -1),
    (0, -1, 1),
    (0, -1, -1),
)
NB = len(OFFSETS)
CORNERS = tuple(b for b in range(NB) if OFFSETS[b][2] == 0)
FACES = tuple(b for b in range(NB) if OFFSETS[b][2] != 0)
FACE_COLUMNS = ((0, -1), (0, 1), (-1, 0), (1, 0))
WEIGHT = 0.125
STEP_SIZE = 0.35
MESH = pl.DeviceIdType.MESH
F32 = jnp.float32
BF16 = jnp.bfloat16


def column(dx, dy):
    return (dx + 1) * 3 + dy + 1


def split(x):
    high = x.astype(BF16)
    return high, (x - high.astype(F32)).astype(BF16)


def left_rows(high, low):
    return jnp.concatenate([high, high, low], axis=1)


def stacked(real, imag, flip):
    rh, rl = split(real)
    ih, il = split(imag)
    if flip:
        high = jnp.concatenate(
            [jnp.concatenate([rh, ih], axis=1), jnp.concatenate([ih, -rh], axis=1)], axis=0
        )
        low = jnp.concatenate(
            [jnp.concatenate([rl, il], axis=1), jnp.concatenate([il, -rl], axis=1)], axis=0
        )
    else:
        high = jnp.concatenate(
            [jnp.concatenate([rh, ih], axis=1), jnp.concatenate([-ih, rh], axis=1)], axis=0
        )
        low = jnp.concatenate(
            [jnp.concatenate([rl, il], axis=1), jnp.concatenate([-il, rl], axis=1)], axis=0
        )
    return jnp.concatenate([high, low, high], axis=0)


def product(left, right):
    return jnp.dot(left, right, preferred_element_type=F32)


def complex_product(left, right_real, right_imag):
    return product(left_rows(*split(left)), stacked(right_real, right_imag, False))


def arctan2(y, x):
    ay = jnp.abs(y)
    ax = jnp.abs(x)
    ratio = jnp.minimum(ax, ay) / jnp.maximum(jnp.maximum(ax, ay), 1e-37)
    far = ratio > 0.4142135623730950
    z = jnp.where(far, (ratio - 1.0) / (ratio + 1.0), ratio)
    s = z * z
    poly = (
        ((8.05374449538e-2 * s - 1.38776856032e-1) * s + 1.99777106478e-1) * s - 3.33329491539e-1
    ) * s * z + z
    angle = jnp.where(far, poly + 0.7853981633974483, poly)
    angle = jnp.where(ay > ax, 1.5707963267948966 - angle, angle)
    angle = jnp.where(x < 0.0, 3.141592653589793 - angle, angle)
    return jnp.where(y < 0.0, -angle, angle)


def signed_sum(rows):
    total = None
    for sign, row in rows:
        if total is None:
            total = row if sign > 0 else -row
        else:
            total = total + row if sign > 0 else total - row
    return total


def kernel(
    sizes,
    total_points,
    u_ref,
    m_ref,
    out_ref,
    centres_ref,
    spreads_ref,
    own,
    halo,
    inter,
    rot,
    uth,
    dre,
    dim,
    gre,
    gim,
    gz,
    gy,
    gx,
    load_u,
    load_m,
    y_send,
    y_recv,
    x_send,
    x_recv,
    f_send,
    f_recv,
    gz_send,
    gz_recv,
    gy_send,
    gy_recv,
    gx_send,
    gx_recv,
):
    nx, ny, nz = sizes
    count = own.shape[1]
    width = own.shape[-1]
    mx = lax.axis_index("kx")
    my = lax.axis_index("ky")
    mz = lax.axis_index("kz")

    def at(dx, dy, dz):
        return (
            lax.rem(mx + (dx + nx), nx),
            lax.rem(my + (dy + ny), ny),
            lax.rem(mz + (dz + nz), nz),
        )

    copy_u = pltpu.make_async_copy(u_ref, own.at[0], load_u)
    copy_u.start()
    for k in range(count):
        pltpu.make_async_copy(m_ref.at[k], inter.at[k], load_m.at[k]).start()

    partners = (
        [at(j, 0, 0) for j in range(1, nx)]
        + [at(0, j, 0) for j in range(1, ny)]
        + [at(0, 0, j) for j in range(1, nz)]
    )
    barrier = pltpu.get_barrier_semaphore()
    for partner in partners:
        pl.semaphore_signal(barrier, inc=1, device_id=partner, device_id_type=MESH)
    pl.semaphore_wait(barrier, len(partners))
    copy_u.wait()

    def remote(src, dst, send, recv, target):
        return pltpu.make_async_remote_copy(
            src_ref=src,
            dst_ref=dst,
            send_sem=send,
            recv_sem=recv,
            device_id=target,
            device_id_type=MESH,
        )

    def y_copy(t, j, k):
        slot = -1 if j == 0 else 1
        return remote(
            own.at[t, k],
            halo.at[t, column(0, slot), k + 1],
            y_send.at[t, j, k],
            y_recv.at[t, j, k],
            at(0, -slot, 0),
        )

    def x_copy(t, i, dy, k):
        slot = -1 if i == 0 else 1
        src = own.at[t, k] if dy == 0 else halo.at[t, column(0, dy), k + 1]
        return remote(
            src,
            halo.at[t, column(slot, dy), k + 1],
            x_send.at[t, i, dy + 1, k],
            x_recv.at[t, i, dy + 1, k],
            at(-slot, 0, 0),
        )

    def f_copy(t, f, side):
        col = column(*FACE_COLUMNS[f])
        if side == 0:
            src, dst, target = 1, count + 1, at(0, 0, -1)
        else:
            src, dst, target = count, 0, at(0, 0, 1)
        return remote(
            halo.at[t, col, src],
            halo.at[t, col, dst],
            f_send.at[t, f, side],
            f_recv.at[t, f, side],
            target,
        )

    row_index = lax.broadcasted_iota(jnp.int32, (width, width), 0)
    column_index = lax.broadcasted_iota(jnp.int32, (width, width), 1)
    diagonal = row_index == column_index
    identity = jnp.where(diagonal, 1.0, 0.0).astype(F32)

    def all_sum(t, axis_slots, send, recv, me, size, target, value):
        axis_slots[t, me] = value
        copies = []
        for j in range(1, size):
            copies.append(
                remote(
                    axis_slots.at[t, me],
                    axis_slots.at[t, me],
                    send.at[t, j],
                    recv.at[t, j],
                    target(j),
                )
            )
            copies[-1].start()
        for j in range(1, size):
            source = lax.rem(me + (size - j), size)
            remote(
                axis_slots.at[t, source],
                axis_slots.at[t, source],
                send.at[t, j],
                recv.at[t, j],
                target(j),
            ).wait_recv()
        for copy in copies:
            copy.wait_send()
        total = axis_slots[t, 0]
        for j in range(1, size):
            total = total + axis_slots[t, j]
        return total

    def turn(t, k, b):
        dx, dy, dz = OFFSETS[b]
        left = rot[k, b]
        right = halo.at[t, column(dx, dy), k + 1 + dz]
        turned = complex_product(left, right[0], right[1])
        rot[k, b] = turned
        dre[k, b : b + 1, :] = jnp.sum(
            jnp.where(diagonal, turned[:, :width], 0.0), axis=0, keepdims=True
        )
        dim[k, b : b + 1, :] = jnp.sum(
            jnp.where(diagonal, turned[:, width:], 0.0), axis=0, keepdims=True
        )

    def iteration(t, carry):
        for k in range(count):
            for j in range(2):
                y_copy(t, j, k).start()
            for i in range(2):
                x_copy(t, i, 0, k).start()

        def left_side(k, carry):
            @pl.when(t == 0)
            def _():
                pltpu.make_async_copy(m_ref.at[k], inter.at[k], load_m.at[k]).wait()

            adjoint = jnp.concatenate([own[t, k, 0].T, own[t, k, 1].T], axis=1)
            uth[...] = left_rows(*split(adjoint))

            def one(b, carry):
                rot[k, b] = product(uth[...], stacked(inter[k, b, 0], inter[k, b, 1], True))
                return carry

            lax.fori_loop(0, NB, one, 0, unroll=3)
            for j in range(2):
                y_copy(t, j, k).wait_recv()
                for i in range(2):
                    x_copy(t, i, -1 if j == 0 else 1, k).start()
            for i in range(2):
                x_copy(t, i, 0, k).wait_recv()

            @pl.when(k == 0)
            def _():
                for f in range(4):
                    f_copy(t, f, 0).start()

            @pl.when(k == count - 1)
            def _():
                for f in range(4):
                    f_copy(t, f, 1).start()

            return carry

        lax.fori_loop(0, count, left_side, 0)
        for f in range(4):
            for side in range(2):
                f_copy(t, f, side).wait_recv()

        def faces(k, carry):
            for b in FACES:
                turn(t, k, b)
            return carry

        lax.fori_loop(0, count, faces, 0)

        def corners(k, carry):
            for i in range(2):
                for dy in (-1, 1):
                    x_copy(t, i, dy, k).wait_recv()
            for b in CORNERS:
                turn(t, k, b)
            return carry

        lax.fori_loop(0, count, corners, 0)

        real = dre[:, :NB, :]
        imag = dim[:, :NB, :]
        phases = arctan2(imag, real)
        magnitude = real * real + imag * imag
        phase_rows = jnp.sum(phases, axis=0)
        second = jnp.sum(
            jnp.sum(1.0 - magnitude + phases * phases, axis=0), axis=0, keepdims=True
        )
        rows = [
            signed_sum(
                [
                    (OFFSETS[b][c], phase_rows[b : b + 1, :])
                    for b in range(NB)
                    if OFFSETS[b][c] != 0
                ]
            )
            for c in range(3)
        ]
        packed = WEIGHT * jnp.concatenate(
            rows + [second] + [jnp.zeros((4, width), F32)], axis=0
        )
        packed = all_sum(t, gz, gz_send, gz_recv, mz, nz, lambda j: at(0, 0, j), packed)
        packed = all_sum(t, gy, gy_send, gy_recv, my, ny, lambda j: at(0, j, 0), packed)
        packed = all_sum(t, gx, gx_send, gx_recv, mx, nx, lambda j: at(j, 0, 0), packed)
        packed = packed / total_points
        centres = -packed[0:3, :]
        spread = packed[3:4, :] - jnp.sum(centres * centres, axis=0, keepdims=True)
        centres_ref[t] = centres
        spreads_ref[t] = spread
        shift = jnp.concatenate(
            [
                signed_sum(
                    [
                        (OFFSETS[b][c], centres[c : c + 1, :])
                        for c in range(3)
                        if OFFSETS[b][c] != 0
                    ]
                )
                for b in range(NB)
            ],
            axis=0,
        )
        scaled = (phases + shift[None]) / magnitude
        gre[:, :NB, :] = real + imag * scaled
        gim[:, :NB, :] = real * scaled - imag

        def update(k, carry):
            summed_real = jnp.zeros((width, width), F32)
            summed_imag = jnp.zeros((width, width), F32)
            for b in range(NB):
                turned_real = rot[k, b, :, :width]
                turned_imag = rot[k, b, :, width:]
                factor_real = gre[k, b : b + 1, :]
                factor_imag = gim[k, b : b + 1, :]
                summed_real = summed_real + (
                    turned_real * factor_real - turned_imag * factor_imag
                )
                summed_imag = summed_imag + (
                    turned_real * factor_imag + turned_imag * factor_real
                )
            scale = STEP_SIZE * 2.0 * WEIGHT
            change_real = scale * (summed_real - summed_real.T)
            change_imag = scale * (summed_imag + summed_imag.T)
            change = left_rows(*split(jnp.concatenate([change_real, change_imag], axis=1)))
            middle = product(
                change,
                stacked(0.5 * identity + change_real / 6.0, change_imag / 6.0, False),
            )
            exponent = product(
                change, stacked(identity + middle[:, :width], middle[:, width:], False)
            )
            updated = complex_product(
                jnp.concatenate([own[t, k, 0], own[t, k, 1]], axis=1),
                identity + exponent[:, :width],
                exponent[:, width:],
            )
            own[t + 1, k, 0] = updated[:, :width]
            own[t + 1, k, 1] = updated[:, width:]
            return carry

        lax.fori_loop(0, count, update, 0)

        def drain(k, carry):
            for j in range(2):
                y_copy(t, j, k).wait_send()
            for i in range(2):
                for dy in (-1, 0, 1):
                    x_copy(t, i, dy, k).wait_send()
            return carry

        lax.fori_loop(0, count, drain, 0)
        for f in range(4):
            for side in range(2):
                f_copy(t, f, side).wait_send()
        return carry

    lax.fori_loop(0, ITERS, iteration, 0)
    out_ref[...] = own[ITERS]


def body(sizes, u_start, intersections):
    nx, ny, nz = sizes
    count_x, count_y, count = u_start.shape[:3]
    width = u_start.shape[-1]
    assert count_x == 1 and count_y == 1
    total_points = count_x * count_y * count * nx * ny * nz
    dma = pltpu.SemaphoreType.DMA
    unitary, centres, spreads = pl.pallas_call(
        functools.partial(kernel, sizes, float(total_points)),
        out_shape=(
            jax.ShapeDtypeStruct((count, 2, width, width), F32),
            jax.ShapeDtypeStruct((ITERS, 3, width), F32),
            jax.ShapeDtypeStruct((ITERS, 1, width), F32),
        ),
        in_specs=[pl.BlockSpec(memory_space=pl.ANY)] * 2,
        out_specs=tuple([pl.BlockSpec(memory_space=pltpu.VMEM)] * 3),
        scratch_shapes=[
            pltpu.VMEM((ITERS + 1, count, 2, width, width), F32),
            pltpu.VMEM((ITERS, 9, count + 2, 2, width, width), F32),
            pltpu.VMEM((count, NB, 2, width, width), F32),
            pltpu.VMEM((count, NB, width, 2 * width), F32),
            pltpu.VMEM((width, 6 * width), BF16),
            pltpu.VMEM((count, 16, width), F32),
            pltpu.VMEM((count, 16, width), F32),
            pltpu.VMEM((count, 16, width), F32),
            pltpu.VMEM((count, 16, width), F32),
            pltpu.VMEM((ITERS, nz, 8, width), F32),
            pltpu.VMEM((ITERS, ny, 8, width), F32),
            pltpu.VMEM((ITERS, nx, 8, width), F32),
            dma,
            dma((count,)),
            dma((ITERS, 2, count)),
            dma((ITERS, 2, count)),
            dma((ITERS, 2, 3, count)),
            dma((ITERS, 2, 3, count)),
            dma((ITERS, 4, 2)),
            dma((ITERS, 4, 2)),
            dma((ITERS, nz)),
            dma((ITERS, nz)),
            dma((ITERS, ny)),
            dma((ITERS, ny)),
            dma((ITERS, nx)),
            dma((ITERS, nx)),
        ],
        compiler_params=pltpu.CompilerParams(
            collective_id=0, has_side_effects=True, vmem_limit_bytes=60 * 1024 * 1024
        ),
    )(
        u_start.reshape(u_start.shape[2:]),
        intersections.reshape(intersections.shape[2:]),
    )
    return unitary.reshape(u_start.shape), centres, spreads.reshape(ITERS, width)


def solution(mesh):
    sizes = (mesh.shape["kx"], mesh.shape["ky"], mesh.shape["kz"])
    in_specs = (P("kx", "ky", "kz", None, None, None), P("kx", "ky", "kz", None, None, None, None))
    out_specs = (P("kx", "ky", "kz", None, None, None), P(), P())
    return jax.shard_map(
        functools.partial(body, sizes),
        mesh=mesh,
        in_specs=in_specs,
        out_specs=out_specs,
        check_vma=False,
    )
```

```python
import functools

import jax
import jax.numpy as jnp
from jax import lax
from jax.experimental import pallas as pl
from jax.experimental.pallas import tpu as pltpu
from jax.sharding import PartitionSpec as P

ITERS = 3


OFFSETS = (
    (1, 1, 0),
    (1, -1, 0),
    (-1, 1, 0),
    (-1, -1, 0),
    (1, 0, 1),
    (1, 0, -1),
    (-1, 0, 1),
    (-1, 0, -1),
    (0, 1, 1),
    (0, 1, -1),
    (0, -1, 1),
    (0, -1, -1),
)
NB = len(OFFSETS)
CORNERS = tuple(b for b in range(NB) if OFFSETS[b][2] == 0)
FACES = tuple(b for b in range(NB) if OFFSETS[b][2] != 0)
FACE_COLUMNS = ((0, -1), (0, 1), (-1, 0), (1, 0))
WEIGHT = 0.125
STEP_SIZE = 0.35
MESH = pl.DeviceIdType.MESH
F32 = jnp.float32
BF16 = jnp.bfloat16


def column(dx, dy):
    return (dx + 1) * 3 + dy + 1


def split(x):
    high = x.astype(BF16)
    return high, (x - high.astype(F32)).astype(BF16)


def left_rows(high, low):
    return jnp.concatenate([high, high, low], axis=1)


def stacked(real, imag, flip):
    rh, rl = split(real)
    ih, il = split(imag)
    if flip:
        high = jnp.concatenate(
            [jnp.concatenate([rh, ih], axis=1), jnp.concatenate([ih, -rh], axis=1)], axis=0
        )
        low = jnp.concatenate(
            [jnp.concatenate([rl, il], axis=1), jnp.concatenate([il, -rl], axis=1)], axis=0
        )
    else:
        high = jnp.concatenate(
            [jnp.concatenate([rh, ih], axis=1), jnp.concatenate([-ih, rh], axis=1)], axis=0
        )
        low = jnp.concatenate(
            [jnp.concatenate([rl, il], axis=1), jnp.concatenate([-il, rl], axis=1)], axis=0
        )
    return jnp.concatenate([high, low, high], axis=0)


def product(left, right):
    return jnp.dot(left, right, preferred_element_type=F32)


def complex_product(left, right_real, right_imag):
    return product(left_rows(*split(left)), stacked(right_real, right_imag, False))


def arctan2(y, x):
    ay = jnp.abs(y)
    ax = jnp.abs(x)
    ratio = jnp.minimum(ax, ay) / jnp.maximum(jnp.maximum(ax, ay), 1e-37)
    far = ratio > 0.4142135623730950
    z = jnp.where(far, (ratio - 1.0) / (ratio + 1.0), ratio)
    s = z * z
    poly = (
        ((8.05374449538e-2 * s - 1.38776856032e-1) * s + 1.99777106478e-1) * s - 3.33329491539e-1
    ) * s * z + z
    angle = jnp.where(far, poly + 0.7853981633974483, poly)
    angle = jnp.where(ay > ax, 1.5707963267948966 - angle, angle)
    angle = jnp.where(x < 0.0, 3.141592653589793 - angle, angle)
    return jnp.where(y < 0.0, -angle, angle)


def signed_sum(rows):
    total = None
    for sign, row in rows:
        if total is None:
            total = row if sign > 0 else -row
        else:
            total = total + row if sign > 0 else total - row
    return total


def kernel(
    sizes,
    total_points,
    u_ref,
    m_ref,
    out_ref,
    centres_ref,
    spreads_ref,
    own,
    expo,
    step,
    halo,
    halo_step,
    inter,
    rot,
    uth,
    dre,
    dim,
    gre,
    gim,
    gz,
    gy,
    gx,
    load_u,
    load_m,
    y_send,
    y_recv,
    x_send,
    x_recv,
    f_send,
    f_recv,
    gz_send,
    gz_recv,
    gy_send,
    gy_recv,
    gx_send,
    gx_recv,
):
    nx, ny, nz = sizes
    count = own.shape[1]
    width = own.shape[-1]
    mx = lax.axis_index("kx")
    my = lax.axis_index("ky")
    mz = lax.axis_index("kz")

    def at(dx, dy, dz):
        return (
            lax.rem(mx + (dx + nx), nx),
            lax.rem(my + (dy + ny), ny),
            lax.rem(mz + (dz + nz), nz),
        )

    copy_u = pltpu.make_async_copy(u_ref, own.at[0], load_u)
    copy_u.start()
    for k in range(count):
        pltpu.make_async_copy(m_ref.at[k], inter.at[k], load_m.at[k]).start()

    partners = (
        [at(j, 0, 0) for j in range(1, nx)]
        + [at(0, j, 0) for j in range(1, ny)]
        + [at(0, 0, j) for j in range(1, nz)]
    )
    barrier = pltpu.get_barrier_semaphore()
    for partner in partners:
        pl.semaphore_signal(barrier, inc=1, device_id=partner, device_id_type=MESH)
    pl.semaphore_wait(barrier, len(partners))
    copy_u.wait()

    def remote(src, dst, send, recv, target):
        return pltpu.make_async_remote_copy(
            src_ref=src,
            dst_ref=dst,
            send_sem=send,
            recv_sem=recv,
            device_id=target,
            device_id_type=MESH,
        )

    def sent(t, k):
        return own.at[0, k] if t == 0 else step.at[t - 1, k]

    def landed(t, col, z):
        return halo.at[col, z] if t == 0 else halo_step.at[t - 1, col, z]

    def y_copy(t, j, dx, k):
        slot = -1 if j == 0 else 1
        return remote(
            sent(t, k) if dx == 0 else landed(t, column(dx, 0), k + 1),
            landed(t, column(dx, slot), k + 1),
            y_send.at[t, j, dx + 1, k],
            y_recv.at[t, j, dx + 1, k],
            at(0, -slot, 0),
        )

    def x_copy(t, i, dy, k):
        slot = -1 if i == 0 else 1
        src = sent(t, k) if dy == 0 else landed(t, column(0, dy), k + 1)
        return remote(
            src,
            landed(t, column(slot, dy), k + 1),
            x_send.at[t, i, dy + 1, k],
            x_recv.at[t, i, dy + 1, k],
            at(-slot, 0, 0),
        )

    def f_copy(t, f, side):
        col = column(*FACE_COLUMNS[f])
        if side == 0:
            src, dst, target = 1, count + 1, at(0, 0, -1)
        else:
            src, dst, target = count, 0, at(0, 0, 1)
        return remote(
            landed(t, col, src),
            landed(t, col, dst),
            f_send.at[t, f, side],
            f_recv.at[t, f, side],
            target,
        )

    row_index = lax.broadcasted_iota(jnp.int32, (width, width), 0)
    column_index = lax.broadcasted_iota(jnp.int32, (width, width), 1)
    diagonal = row_index == column_index
    identity = jnp.where(diagonal, 1.0, 0.0).astype(F32)

    def all_sum(t, axis_slots, send, recv, me, size, target, value):
        axis_slots[t, me] = value
        copies = []
        for j in range(1, size):
            copies.append(
                remote(
                    axis_slots.at[t, me],
                    axis_slots.at[t, me],
                    send.at[t, j],
                    recv.at[t, j],
                    target(j),
                )
            )
            copies[-1].start()
        for j in range(1, size):
            source = lax.rem(me + (size - j), size)
            remote(
                axis_slots.at[t, source],
                axis_slots.at[t, source],
                send.at[t, j],
                recv.at[t, j],
                target(j),
            ).wait_recv()
        for copy in copies:
            copy.wait_send()
        total = axis_slots[t, 0]
        for j in range(1, size):
            total = total + axis_slots[t, j]
        return total

    def unpacked(values):
        flipped = values.T
        real = jnp.where(row_index < column_index, values, -flipped)
        return (
            jnp.where(diagonal, 0.0, real),
            jnp.where(row_index < column_index, flipped, values),
        )

    def exponential(change_real, change_imag):
        change = left_rows(*split(jnp.concatenate([change_real, change_imag], axis=1)))
        middle = product(
            change,
            stacked(0.5 * identity + change_real / 6.0, change_imag / 6.0, False),
        )
        exponent = product(
            change, stacked(identity + middle[:, :width], middle[:, width:], False)
        )
        return identity + exponent[:, :width], exponent[:, width:]

    def via_x(k):
        return lax.rem(k, 2) == 0

    def turn(t, k, b):
        dx, dy, dz = OFFSETS[b]
        left = rot[k, b]
        right = landed(t, column(dx, dy), k + 1 + dz)
        if t == 0:
            turned = complex_product(left, right[0], right[1])
        else:
            turned = complex_product(left, *exponential(*unpacked(right[...])))
        rot[k, b] = turned
        dre[k, b : b + 1, :] = jnp.sum(
            jnp.where(diagonal, turned[:, :width], 0.0), axis=0, keepdims=True
        )
        dim[k, b : b + 1, :] = jnp.sum(
            jnp.where(diagonal, turned[:, width:], 0.0), axis=0, keepdims=True
        )

    def iteration(t):
        for k in range(count):
            for j in range(2):
                y_copy(t, j, 0, k).start()
            for i in range(2):
                x_copy(t, i, 0, k).start()

        def left_side(k, carry):
            if t == 0:
                pltpu.make_async_copy(m_ref.at[k], inter.at[k], load_m.at[k]).wait()
                adjoint = jnp.concatenate([own[t, k, 0].T, own[t, k, 1].T], axis=1)
            else:
                adjoint = jnp.concatenate([expo[k, 0].T, expo[k, 1].T], axis=1)
            uth[...] = left_rows(*split(adjoint))

            def one(b, carry):
                if t == 0:
                    real, imag = inter[k, b, 0], inter[k, b, 1]
                else:
                    real, imag = rot[k, b, :, :width], rot[k, b, :, width:]
                rot[k, b] = product(uth[...], stacked(real, imag, True))
                return carry

            lax.fori_loop(0, NB, one, 0, unroll=3)
            for j in range(2):
                y_copy(t, j, 0, k).wait_recv()

            @pl.when(via_x(k))
            def _():
                for i in range(2):
                    for dy in (-1, 1):
                        x_copy(t, i, dy, k).start()

            for i in range(2):
                x_copy(t, i, 0, k).wait_recv()

            @pl.when(jnp.logical_not(via_x(k)))
            def _():
                for j in range(2):
                    for dx in (-1, 1):
                        y_copy(t, j, dx, k).start()

            @pl.when(k == 0)
            def _():
                for f in range(4):
                    f_copy(t, f, 0).start()

            @pl.when(k == count - 1)
            def _():
                for f in range(4):
                    f_copy(t, f, 1).start()

            return carry

        lax.fori_loop(0, count, left_side, 0)
        for f in range(4):
            for side in range(2):
                f_copy(t, f, side).wait_recv()

        def faces(k, carry):
            for b in FACES:
                turn(t, k, b)
            return carry

        lax.fori_loop(0, count, faces, 0)

        def corners(k, carry):
            @pl.when(via_x(k))
            def _():
                for i in range(2):
                    for dy in (-1, 1):
                        x_copy(t, i, dy, k).wait_recv()

            @pl.when(jnp.logical_not(via_x(k)))
            def _():
                for j in range(2):
                    for dx in (-1, 1):
                        y_copy(t, j, dx, k).wait_recv()

            for b in CORNERS:
                turn(t, k, b)
            return carry

        lax.fori_loop(0, count, corners, 0)

        real = dre[:, :NB, :]
        imag = dim[:, :NB, :]
        phases = arctan2(imag, real)
        magnitude = real * real + imag * imag
        phase_rows = jnp.sum(phases, axis=0)
        second = jnp.sum(
            jnp.sum(1.0 - magnitude + phases * phases, axis=0), axis=0, keepdims=True
        )
        rows = [
            signed_sum(
                [
                    (OFFSETS[b][c], phase_rows[b : b + 1, :])
                    for b in range(NB)
                    if OFFSETS[b][c] != 0
                ]
            )
            for c in range(3)
        ]
        packed = WEIGHT * jnp.concatenate(
            rows + [second] + [jnp.zeros((4, width), F32)], axis=0
        )
        packed = all_sum(t, gz, gz_send, gz_recv, mz, nz, lambda j: at(0, 0, j), packed)
        packed = all_sum(t, gy, gy_send, gy_recv, my, ny, lambda j: at(0, j, 0), packed)
        packed = all_sum(t, gx, gx_send, gx_recv, mx, nx, lambda j: at(j, 0, 0), packed)
        packed = packed / total_points
        centres = -packed[0:3, :]
        spread = packed[3:4, :] - jnp.sum(centres * centres, axis=0, keepdims=True)
        centres_ref[t] = centres
        spreads_ref[t] = spread
        shift = jnp.concatenate(
            [
                signed_sum(
                    [
                        (OFFSETS[b][c], centres[c : c + 1, :])
                        for c in range(3)
                        if OFFSETS[b][c] != 0
                    ]
                )
                for b in range(NB)
            ],
            axis=0,
        )
        scaled = (phases + shift[None]) / magnitude
        gre[:, :NB, :] = real + imag * scaled
        gim[:, :NB, :] = real * scaled - imag

        def update(k, carry):
            summed_real = jnp.zeros((width, width), F32)
            summed_imag = jnp.zeros((width, width), F32)
            for b in range(NB):
                turned_real = rot[k, b, :, :width]
                turned_imag = rot[k, b, :, width:]
                factor_real = gre[k, b : b + 1, :]
                factor_imag = gim[k, b : b + 1, :]
                summed_real = summed_real + (
                    turned_real * factor_real - turned_imag * factor_imag
                )
                summed_imag = summed_imag + (
                    turned_real * factor_imag + turned_imag * factor_real
                )
            scale = STEP_SIZE * 2.0 * WEIGHT
            change_real = scale * (summed_real - summed_real.T)
            change_imag = scale * (summed_imag + summed_imag.T)
            expo_real, expo_imag = exponential(change_real, change_imag)
            if t < ITERS - 1:
                step[t, k] = jnp.where(row_index < column_index, change_real, change_imag)
                expo[k, 0] = expo_real
                expo[k, 1] = expo_imag
            updated = complex_product(
                jnp.concatenate([own[t, k, 0], own[t, k, 1]], axis=1), expo_real, expo_imag
            )
            own[t + 1, k, 0] = updated[:, :width]
            own[t + 1, k, 1] = updated[:, width:]
            return carry

        lax.fori_loop(0, count, update, 0)

        def drain(k, carry):
            for j in range(2):
                y_copy(t, j, 0, k).wait_send()
            for i in range(2):
                x_copy(t, i, 0, k).wait_send()

            @pl.when(via_x(k))
            def _():
                for i in range(2):
                    for dy in (-1, 1):
                        x_copy(t, i, dy, k).wait_send()

            @pl.when(jnp.logical_not(via_x(k)))
            def _():
                for j in range(2):
                    for dx in (-1, 1):
                        y_copy(t, j, dx, k).wait_send()

            return carry

        lax.fori_loop(0, count, drain, 0)
        for f in range(4):
            for side in range(2):
                f_copy(t, f, side).wait_send()

    for t in range(ITERS):
        iteration(t)
    out_ref[...] = own[ITERS]


def body(sizes, u_start, intersections):
    nx, ny, nz = sizes
    count_x, count_y, count = u_start.shape[:3]
    width = u_start.shape[-1]
    assert count_x == 1 and count_y == 1
    total_points = count_x * count_y * count * nx * ny * nz
    dma = pltpu.SemaphoreType.DMA
    unitary, centres, spreads = pl.pallas_call(
        functools.partial(kernel, sizes, float(total_points)),
        out_shape=(
            jax.ShapeDtypeStruct((count, 2, width, width), F32),
            jax.ShapeDtypeStruct((ITERS, 3, width), F32),
            jax.ShapeDtypeStruct((ITERS, 1, width), F32),
        ),
        in_specs=[pl.BlockSpec(memory_space=pl.ANY)] * 2,
        out_specs=tuple([pl.BlockSpec(memory_space=pltpu.VMEM)] * 3),
        scratch_shapes=[
            pltpu.VMEM((ITERS + 1, count, 2, width, width), F32),
            pltpu.VMEM((count, 2, width, width), F32),
            pltpu.VMEM((ITERS - 1, count, width, width), F32),
            pltpu.VMEM((9, count + 2, 2, width, width), F32),
            pltpu.VMEM((ITERS - 1, 9, count + 2, width, width), F32),
            pltpu.VMEM((count, NB, 2, width, width), F32),
            pltpu.VMEM((count, NB, width, 2 * width), F32),
            pltpu.VMEM((width, 6 * width), BF16),
            pltpu.VMEM((count, 16, width), F32),
            pltpu.VMEM((count, 16, width), F32),
            pltpu.VMEM((count, 16, width), F32),
            pltpu.VMEM((count, 16, width), F32),
            pltpu.VMEM((ITERS, nz, 8, width), F32),
            pltpu.VMEM((ITERS, ny, 8, width), F32),
            pltpu.VMEM((ITERS, nx, 8, width), F32),
            dma,
            dma((count,)),
            dma((ITERS, 2, 3, count)),
            dma((ITERS, 2, 3, count)),
            dma((ITERS, 2, 3, count)),
            dma((ITERS, 2, 3, count)),
            dma((ITERS, 4, 2)),
            dma((ITERS, 4, 2)),
            dma((ITERS, nz)),
            dma((ITERS, nz)),
            dma((ITERS, ny)),
            dma((ITERS, ny)),
            dma((ITERS, nx)),
            dma((ITERS, nx)),
        ],
        compiler_params=pltpu.CompilerParams(
            collective_id=0, has_side_effects=True, vmem_limit_bytes=60 * 1024 * 1024
        ),
    )(
        u_start.reshape(u_start.shape[2:]),
        intersections.reshape(intersections.shape[2:]),
    )
    return unitary.reshape(u_start.shape), centres, spreads.reshape(ITERS, width)


def solution(mesh):
    sizes = (mesh.shape["kx"], mesh.shape["ky"], mesh.shape["kz"])
    in_specs = (P("kx", "ky", "kz", None, None, None), P("kx", "ky", "kz", None, None, None, None))
    out_specs = (P("kx", "ky", "kz", None, None, None), P(), P())
    return jax.shard_map(
        functools.partial(body, sizes),
        mesh=mesh,
        in_specs=in_specs,
        out_specs=out_specs,
        check_vma=False,
    )
```
